32 devices in a mesh: frame: 8 (over z, y), clip: 4 (over x, core).
Axes of the slice: x: 2, y: 2, z: 4, core: 2. Of those that a mesh axis runs over, the one named last changes fastest.
Arguments:
- tokens: bfloat16 [4, 64, 2, 49, 256], P('clip', 'frame'), may hold values from -6 to 6
- lengths: int32 [4], P('clip'), may hold values from 32 to 64, as said below
- norm_gain: float32 [256], replicated, may hold values from 0.25 to 1.75
- norm_bias: float32 [256], replicated, may hold values from -1.5 to 1.5
- qkv_weight: float32 [256, 768], replicated, may hold values from -0.375 to 0.375
- qkv_bias: float32 [768], replicated, may hold values from -1.5 to 1.5
- proj_weight: float32 [256, 256], replicated, may hold values from -0.375 to 0.375
- proj_bias: float32 [256], replicated, may hold values from -1.5 to 1.5
- grad_out: bfloat16 [4, 64, 2, 49, 256], P('clip', 'frame'), may hold values from -6 to 6
Outputs:
- mixed: bfloat16 [4, 64, 2, 49, 256], P('clip', 'frame')
- grad_tokens: bfloat16 [4, 64, 2, 49, 256], P('clip', 'frame')
- grad_gain: float32 [256], replicated
- grad_nbias: float32 [256], replicated
- grad_qkv_weight: float32 [256, 768], replicated
- grad_qkv_bias: float32 [768], replicated
- grad_proj_weight: float32 [256, 256], replicated
- grad_proj_bias: float32 [256], replicated
The draws below stay inside these ranges and needn't reach their ends.
Inputs may be any that keep to these rules, and one draw needn't show every extreme that they name: `lengths`: each clip has at least 32 frames that are not padding, and at least one clip has all 64 frames.
All inputs are finite; a program needn't handle non-finite values.
Results may differ from the reference program's by a relative error of at most 0.012.
Values may be sent and summed in bfloat16 or wider, within the bound.
A program may use at most 192 MiB of HBM per device.

```python
import jax
import jax.numpy as jnp
from jax import lax

D = 256
HEADS = 8
WT = 8
PATCH = 49
WIN_DEV = 2
FRAMES = 64
CLIPS = 4
N_FRAME = 8


def draw_lengths(key, part):
    base_key = jax.random.fold_in(key, 11)
    pick_key = jax.random.fold_in(key, 23)
    base = jax.random.randint(base_key, (CLIPS,), FRAMES // 2, FRAMES + 1, dtype=jnp.int32)
    chosen = jax.random.randint(pick_key, (), 0, CLIPS, dtype=jnp.int32)
    return jnp.where(jnp.arange(CLIPS, dtype=jnp.int32) == chosen, jnp.int32(FRAMES), base).astype(jnp.int32)


def steps_of(stream_key, extent, pieces, smallest, largest):
    def one(dim, blocks):
        heights = jax.random.uniform(jax.random.fold_in(jax.random.fold_in(stream_key, 6), dim), (blocks,), jnp.float32, smallest / len(pieces), largest / len(pieces))
        return jnp.repeat(jnp.exp(heights), extent[dim] // blocks).reshape((-1,) + (1,) * (len(extent) - dim - 1))

    level = one(*pieces[0])
    for cut in pieces[1:]:
        level = level * one(*cut)
    return level


def centred(key, extent, spread, bound, shards=(), kind=jnp.bfloat16):
    gain = steps_of(key, extent, shards, -0.22, 0.18) if shards else 1.0
    array = jax.random.normal(key, extent, jnp.float32) * spread * gain
    return jnp.minimum(jnp.maximum(array, -bound), bound).astype(kind)


def setup_inputs(seed: int = 0) -> dict:
    keys = jax.random.split(jax.random.key(seed), 10)
    tokens = centred(keys[0], (CLIPS, FRAMES, WIN_DEV, PATCH, D), 1.0, 6.0, ((0, 4), (1, 8)))
    lengths = draw_lengths(jax.random.fold_in(keys[9], 71), 0)
    norm_gain = jnp.clip(1.0 + 0.15 * jax.random.normal(keys[2], (D,), jnp.float32), 0.25, 1.75)
    norm_bias = centred(keys[3], (D,), 0.3, 1.5, (), jnp.float32)
    qkv_weight = centred(keys[4], (D, 3 * D), D ** -0.5, 0.375, (), jnp.float32)
    qkv_bias = centred(keys[5], (3 * D,), 0.3, 1.5, (), jnp.float32)
    proj_weight = centred(keys[6], (D, D), D ** -0.5, 0.375, (), jnp.float32)
    proj_bias = centred(keys[7], (D,), 0.3, 1.5, (), jnp.float32)
    grad_out = centred(keys[8], (CLIPS, FRAMES, WIN_DEV, PATCH, D), 1.0, 6.0, ((0, 4), (1, 8)))
    return {"tokens": tokens, "lengths": lengths, "norm_gain": norm_gain, "norm_bias": norm_bias, "qkv_weight": qkv_weight, "qkv_bias": qkv_bias, "proj_weight": proj_weight, "proj_bias": proj_bias, "grad_out": grad_out}


def branch(slab, length, first_frame, frame_total, norm_gain, norm_bias, qkv_weight, qkv_bias, proj_weight, proj_bias):
    frames, windows, patch_len, model_width = slab.shape
    head_count = HEADS
    head_depth = model_width // head_count
    offset = WT // 2
    frame_index = jnp.mod(first_frame + jnp.arange(frames, dtype=jnp.int32), frame_total)
    valid_frame = frame_index < length
    region = frame_index < offset
    values = slab.astype(jnp.float32)
    mean_val = lax.optimization_barrier(jnp.mean(values, axis=-1, keepdims=True))
    variance = lax.optimization_barrier(jnp.mean((values - mean_val) ** 2, axis=-1, keepdims=True))
    normed = ((values - mean_val) * lax.rsqrt(variance + 1e-05) * norm_gain + norm_bias).astype(jnp.bfloat16)
    project_qkv = jnp.dot(normed.reshape(-1, model_width), qkv_weight.astype(jnp.bfloat16), preferred_element_type=jnp.float32) + qkv_bias
    project_qkv = project_qkv.astype(jnp.bfloat16)
    time_windows = frames // WT
    project_qkv = project_qkv.reshape(time_windows, WT, windows, patch_len, 3, head_count, head_depth)
    project_qkv = project_qkv.transpose(4, 0, 2, 5, 1, 3, 6).reshape(3, time_windows, windows, head_count, WT * patch_len, head_depth)
    queries = project_qkv[0].astype(jnp.float32)
    keys_f = project_qkv[1].astype(jnp.float32)
    values_f = project_qkv[2].astype(jnp.float32)
    key_valid = jnp.repeat(valid_frame.reshape(time_windows, WT), patch_len, axis=1)
    key_region = jnp.repeat(region.reshape(time_windows, WT), patch_len, axis=1)
    allowed = key_valid[:, None, :] & (key_region[:, :, None] == key_region[:, None, :])
    scores = jnp.einsum('nwhqe,nwhke->nwhqk', queries, keys_f) * head_depth ** (-0.5)
    scores = jnp.where(allowed[:, None, None], scores, -1000000000.0)
    attn_probs = jax.nn.softmax(scores, axis=-1).astype(jnp.bfloat16)
    attended = jnp.einsum('nwhqk,nwhke->nwhqe', attn_probs.astype(jnp.float32), values_f).astype(jnp.bfloat16)
    attended = attended.reshape(time_windows, windows, head_count, WT, patch_len, head_depth)
    attended = attended.transpose(0, 3, 1, 4, 2, 5).reshape(-1, model_width)
    projected = jnp.dot(attended, proj_weight.astype(jnp.bfloat16), preferred_element_type=jnp.float32) + proj_bias
    projected = projected.reshape(frames, windows, patch_len, model_width) * valid_frame.astype(jnp.float32)[:, None, None, None]
    return projected.astype(jnp.bfloat16)

def reference(tokens, lengths, norm_gain, norm_bias, qkv_weight, qkv_bias, proj_weight, proj_bias, grad_out):
    offset = WT // 2
    params = (norm_gain, norm_bias, qkv_weight, qkv_bias, proj_weight, proj_bias)
    clips = tokens.shape[0]
    frame_total = tokens.shape[1]
    frames_dev = frame_total // N_FRAME
    tail_shape = tokens.shape[2:]
    rolled = jnp.roll(tokens, -offset, axis=1).reshape((clips * N_FRAME, frames_dev) + tail_shape)
    grad_slabs = jnp.roll(grad_out, -offset, axis=1).reshape((clips * N_FRAME, frames_dev) + tail_shape)

    def per_slab(operands):
        slab, grad_slab, slab_index = operands
        clip_index = slab_index // N_FRAME
        frame_slot = slab_index % N_FRAME
        length = lengths[clip_index]
        first_frame = frame_slot * frames_dev + offset

        def local_fn(slab_in, param_set):
            return branch(slab_in, length, first_frame, frame_total, *param_set)
        branch_out, pullback = jax.vjp(local_fn, slab, params)
        grad_rolled, grad_params = pullback(grad_slab)
        return (branch_out, grad_rolled, tuple((g.astype(jnp.float32) for g in grad_params)))
    branch_out, grad_rolled, grad_params = lax.map(per_slab, (rolled, grad_slabs, jnp.arange(clips * N_FRAME, dtype=jnp.int32)))
    summed = tuple((lax.optimization_barrier(jnp.sum(g, axis=0)) for g in grad_params))
    branch_full = jnp.roll(branch_out.reshape(tokens.shape), offset, axis=1)
    grad_back = jnp.roll(grad_rolled.reshape(tokens.shape), offset, axis=1)
    mixed = (tokens.astype(jnp.float32) + branch_full.astype(jnp.float32)).astype(jnp.bfloat16)
    grad_tokens = grad_out + grad_back
    return (mixed, grad_tokens, summed[0], summed[1], summed[2], summed[3], summed[4], summed[5])
```

```python
import functools

import jax
import jax.numpy as jnp
from jax import lax
from jax.experimental import pallas as pl
from jax.experimental.pallas import tpu as pltpu
from jax.sharding import PartitionSpec as P

HEADS = 8
WT = 8
MESH = pl.DeviceIdType.MESH
F32 = jnp.float32
BF16 = jnp.bfloat16


def dot(a, b):
    return jnp.dot(a, b, preferred_element_type=F32)


def dot_nt(a, b):
    return lax.dot_general(a, b, (((1,), (1,)), ((), ())), preferred_element_type=F32)


def compute_kernel(
    patch,
    scal,
    x_own,
    x_ahead,
    g_own,
    g_ahead,
    gain,
    nbias,
    wqkv,
    bqkv,
    wproj,
    bproj,
    b_keep,
    b_send,
    d_keep,
    d_send,
    big,
    small,
    xs,
    gs,
    wq16,
    wp16,
    mask,
    probs,
    q16,
    k16,
    v16,
    qt16,
    kt16,
    vt16,
    do16,
    dot16,
    acc_o,
    acc_q,
    dkt,
    dvt,
    acc_big,
):
    step = pl.program_id(0)
    half = WT // 2
    padded = xs.shape[1]
    rows = WT * padded
    width = xs.shape[2]
    depth = width // HEADS
    scale = depth ** (-0.5)
    length = scal[0].astype(F32)
    first = scal[1].astype(F32)
    total = scal[2].astype(F32)
    far = F32(-1e9)

    def frame_of(index):
        row = index.astype(F32)
        slot = jnp.floor((row + 0.5) * (1.0 / padded))
        time = first + slot
        time = jnp.where(time >= total, time - total, time)
        return time, row - slot * padded

    t_col, in_col = frame_of(lax.broadcasted_iota(jnp.int32, (rows, 1), 0))
    valid_col = jnp.where(t_col < length, 1.0, 0.0).astype(F32)

    @pl.when(step == 0)
    def _():
        xs[...] = jnp.zeros_like(xs)
        gs[...] = jnp.zeros_like(gs)
        wq16[...] = wqkv[...].astype(BF16)
        wp16[...] = wproj[...].astype(BF16)
        acc_big[...] = jnp.zeros_like(acc_big)
        small[...] = jnp.zeros_like(small)
        t_row, in_row = frame_of(lax.broadcasted_iota(jnp.int32, (1, rows), 1))
        key_bias = jnp.where((t_row < length) & (in_row < patch), 0.0, far)
        region_row = jnp.where(t_row < half, 1.0, 0.0)
        region_col = jnp.where(t_col < half, 1.0, 0.0)
        mask[...] = key_bias + jnp.where(region_col == region_row, 0.0, far)

    xs[0:half, 0:patch, :] = x_own[0, :, 0].astype(F32)
    xs[half:WT, 0:patch, :] = x_ahead[0, :, 0].astype(F32)
    gs[0:half, 0:patch, :] = g_own[0, :, 0].astype(F32)
    gs[half:WT, 0:patch, :] = g_ahead[0, :, 0].astype(F32)

    x = xs[...].reshape(rows, width)
    mean = jnp.sum(x, axis=-1, keepdims=True) * (1.0 / width)
    xc = x - mean
    var = jnp.sum(xc * xc, axis=-1, keepdims=True) * (1.0 / width)
    inv = lax.rsqrt(var + 1e-05)
    normed_f = (xc * inv * gain[...] + nbias[...]).astype(BF16).astype(F32)
    normed = normed_f.astype(BF16)
    normed_t = normed_f.T.astype(BF16)
    for part, (ref, ref_t) in enumerate(((q16, qt16), (k16, kt16), (v16, vt16))):
        cols = slice(part * width, (part + 1) * width)
        value = dot(normed, wq16[:, cols]) + bqkv[:, cols]
        rounded = value.astype(BF16)
        ref[...] = rounded
        ref_t[...] = rounded.astype(F32).T.astype(BF16)

    lane_head = lax.broadcasted_iota(jnp.int32, (1, width), 1) // depth
    row_head = lax.broadcasted_iota(jnp.int32, (width, 1), 0) // depth
    zero16 = jnp.zeros((), BF16)

    acc_o[...] = jnp.zeros_like(acc_o)

    def forward(h, carry):
        row_on = jnp.where(row_head == h, 1.0, 0.0).astype(BF16)
        lane_on = jnp.where(lane_head == h, 1.0, 0.0).astype(BF16)
        scores = dot(q16[...], kt16[...] * row_on) * scale + mask[...]
        top = jnp.max(scores, axis=-1, keepdims=True)
        e = jnp.exp(scores - top)
        p = (e * (1.0 / jnp.sum(e, axis=-1, keepdims=True))).astype(BF16)
        probs[h] = p
        acc_o[...] += dot(p, v16[...] * lane_on)
        return carry

    lax.fori_loop(0, HEADS, forward, 0, unroll=2)
    att = acc_o[...].astype(BF16)
    att_f = att.astype(F32)
    projected = (dot(att, wp16[...]) + bproj[...]) * valid_col
    projected = projected.reshape(WT, padded, width)
    b_keep[0, :, 0] = projected[0:half, 0:patch].astype(BF16)
    b_send[0, :, 0] = projected[half:WT, 0:patch].astype(BF16)

    g = gs[...].reshape(rows, width) * valid_col
    g_16 = g.astype(BF16)
    small[5:6, :] += jnp.sum(g, axis=0, keepdims=True)
    acc_big[3 * width : 4 * width, :] += dot(att_f.T.astype(BF16), g_16)
    d_att = dot_nt(g_16, wp16[...]).astype(BF16)
    do16[...] = d_att
    d_att_f = d_att.astype(F32)
    dot16[...] = d_att_f.T.astype(BF16)
    acc_o[...] = d_att_f * att_f
    acc_q[...] = jnp.zeros_like(acc_q)

    def backward(h, carry):
        row_on = jnp.where(row_head == h, 1.0, 0.0).astype(BF16)
        lane_on = jnp.where(lane_head == h, 1.0, 0.0).astype(BF16)
        delta = jnp.sum(
            jnp.where(lane_head == h, acc_o[...], 0.0), axis=-1, keepdims=True
        )
        p = probs[h]
        dp = dot(do16[...], vt16[...] * row_on)
        ds = (p.astype(F32) * (dp - delta)).astype(BF16)
        acc_q[...] += dot(ds, k16[...] * lane_on)
        at = pl.ds(pl.multiple_of(h * depth, depth), depth)
        dkt[at, :] = dot(qt16[at, :], ds)
        dvt[at, :] = dot(dot16[at, :], p)
        return carry

    lax.fori_loop(0, HEADS, backward, 0, unroll=2)
    d_normed = jnp.zeros((rows, width), F32)
    for part in range(3):
        if part == 0:
            d_part = acc_q[...] * scale
        elif part == 1:
            d_part = dkt[...].T * scale
        else:
            d_part = dvt[...].T
        d_16 = d_part.astype(BF16)
        cols = slice(part * width, (part + 1) * width)
        small[2 + part : 3 + part, :] += jnp.sum(d_16.astype(F32), axis=0, keepdims=True)
        acc_big[cols, :] += dot(normed_t, d_16)
        d_normed = d_normed + dot_nt(d_16, wq16[:, cols])
    dn = d_normed.astype(BF16).astype(F32)
    x = xs[...].reshape(rows, width)
    xhat = (x - mean) * inv
    small[0:1, :] += jnp.sum(dn * xhat, axis=0, keepdims=True)
    small[1:2, :] += jnp.sum(dn, axis=0, keepdims=True)
    dh = dn * gain[...]
    m1 = jnp.sum(dh, axis=-1, keepdims=True) * (1.0 / width)
    m2 = jnp.sum(dh * xhat, axis=-1, keepdims=True) * (1.0 / width)
    dx = (inv * (dh - m1 - xhat * m2)).reshape(WT, padded, width)
    d_keep[0, :, 0] = dx[0:half, 0:patch].astype(BF16)
    d_send[0, :, 0] = dx[half:WT, 0:patch].astype(BF16)

    @pl.when(step == pl.num_programs(0) - 1)
    def _():
        big[...] = acc_big[...].astype(BF16)


def compute(scal, tokens, ahead, grad_out, ahead_grad, params):
    gain, nbias, wqkv, bqkv, wproj, bproj = params
    _, frames, windows, patch, width = tokens.shape
    half = WT // 2
    padded = -(-patch // 8) * 8
    rows = WT * padded
    own = pl.BlockSpec((1, half, 1, patch, width), lambda w: (0, 1, w, 0, 0))
    other = pl.BlockSpec((1, half, 1, patch, width), lambda w: (0, 0, w, 0, 0))

    def whole(shape):
        return pl.BlockSpec(shape, lambda w: (0,) * len(shape))

    half_shape = jax.ShapeDtypeStruct((1, half, windows, patch, width), BF16)
    tall = pltpu.VMEM((rows, width), BF16)
    wide = pltpu.VMEM((width, rows), BF16)
    return pl.pallas_call(
        functools.partial(compute_kernel, patch),
        grid=(windows,),
        out_shape=[half_shape] * 4
        + [
            jax.ShapeDtypeStruct((4 * width, width), BF16),
            jax.ShapeDtypeStruct((8, width), F32),
        ],
        in_specs=[
            pl.BlockSpec(memory_space=pltpu.SMEM),
            own,
            other,
            own,
            other,
            whole((1, width)),
            whole((1, width)),
            whole((width, 3 * width)),
            whole((1, 3 * width)),
            whole((width, width)),
            whole((1, width)),
        ],
        out_specs=[other] * 4 + [whole((4 * width, width)), whole((8, width))],
        scratch_shapes=[
            pltpu.VMEM((WT, padded, width), F32),
            pltpu.VMEM((WT, padded, width), F32),
            pltpu.VMEM((width, 3 * width), BF16),
            pltpu.VMEM((width, width), BF16),
            pltpu.VMEM((rows, rows), F32),
            pltpu.VMEM((HEADS, rows, rows), BF16),
            tall,
            tall,
            tall,
            wide,
            wide,
            wide,
            tall,
            wide,
            pltpu.VMEM((rows, width), F32),
            pltpu.VMEM((rows, width), F32),
            pltpu.VMEM((width, rows), F32),
            pltpu.VMEM((width, rows), F32),
            pltpu.VMEM((4 * width, width), F32),
        ],
        compiler_params=pltpu.CompilerParams(
            dimension_semantics=("arbitrary",), vmem_limit_bytes=56 * 2**20
        ),
        name="window_attention",
    )(
        scal,
        tokens,
        ahead,
        grad_out,
        ahead_grad,
        gain.reshape(1, width),
        nbias.reshape(1, width),
        wqkv,
        bqkv.reshape(1, 3 * width),
        wproj,
        bproj.reshape(1, width),
    )


def halo_kernel(n_frame, tokens, grads, got_tokens, got_grads, send_sem, recv_sem):
    frame, clip = lax.axis_index("frame"), lax.axis_index("clip")
    before = (lax.rem(frame + n_frame - 1, n_frame), clip)
    after = (lax.rem(frame + 1, n_frame), clip)
    barrier = pltpu.get_barrier_semaphore()
    for peer in (before, after):
        pl.semaphore_signal(barrier, inc=1, device_id=peer, device_id_type=MESH)
    pl.semaphore_wait(barrier, 2)
    half = WT // 2
    copies = []
    for i, (src, dst) in enumerate(((tokens, got_tokens), (grads, got_grads))):
        copy = pltpu.make_async_remote_copy(
            src_ref=src.at[:, 0:half],
            dst_ref=dst,
            send_sem=send_sem.at[i],
            recv_sem=recv_sem.at[i],
            device_id=before,
            device_id_type=MESH,
        )
        copy.start()
        copies.append(copy)
    for copy in copies:
        copy.wait()


def halo(tokens, grad_out, n_frame):
    _, _, windows, patch, width = tokens.shape
    shape = jax.ShapeDtypeStruct((1, WT // 2, windows, patch, width), BF16)
    anywhere = pl.BlockSpec(memory_space=pl.ANY)
    return pl.pallas_call(
        functools.partial(halo_kernel, n_frame),
        out_shape=[shape, shape],
        in_specs=[anywhere] * 2,
        out_specs=[anywhere] * 2,
        scratch_shapes=[pltpu.SemaphoreType.DMA((2,)), pltpu.SemaphoreType.DMA((2,))],
        compiler_params=pltpu.CompilerParams(collective_id=0, has_side_effects=True),
        name="halo",
    )(tokens, grad_out)


def finish_kernel(
    n_frame,
    n_clip,
    branch,
    grads,
    big,
    small,
    got_branch,
    got_grads,
    out_big,
    out_small,
    clip_recv,
    clip_small,
    clip_sum,
    frame_recv,
    frame_small,
    piece,
    h_send,
    h_recv,
    c_send,
    c_recv,
    f_send,
    f_recv,
    a_send,
    a_recv,
    z_send,
    z_recv,
):
    frame, clip = lax.axis_index("frame"), lax.axis_index("clip")
    after = lax.rem(frame + 1, n_frame)
    barrier = pltpu.get_barrier_semaphore()

    def frame_peer(k):
        return lax.rem(frame + k, n_frame)

    def clip_peer(k):
        return lax.rem(clip + k, n_clip)

    for k in range(1, n_clip):
        pl.semaphore_signal(
            barrier, inc=1, device_id=(frame, clip_peer(k)), device_id_type=MESH
        )
    for k in range(1, n_frame):
        pl.semaphore_signal(
            barrier, inc=1, device_id=(frame_peer(k), clip), device_id_type=MESH
        )
    pl.semaphore_wait(barrier, n_clip + n_frame - 2)

    def send(src, dst, s, r, peer):
        copy = pltpu.make_async_remote_copy(
            src_ref=src,
            dst_ref=dst,
            send_sem=s,
            recv_sem=r,
            device_id=peer,
            device_id_type=MESH,
        )
        copy.start()
        return copy

    first = []
    for k in range(1, n_clip):
        peer = (frame, clip_peer(k))
        first.append(
            send(big.at[clip_peer(k)], clip_recv.at[k - 1], c_send.at[0, k], c_recv.at[0, k], peer)
        )
        first.append(send(small, clip_small.at[clip], c_send.at[1, k], c_recv.at[1, k], peer))
    halos = [
        send(branch, got_branch, h_send.at[0], h_recv.at[0], (after, clip)),
        send(grads, got_grads, h_send.at[1], h_recv.at[1], (after, clip)),
    ]
    clip_small[clip] = small[...]
    for copy in first:
        copy.wait()
    total = big[clip].astype(F32)
    for k in range(1, n_clip):
        total = total + clip_recv[k - 1].astype(F32)
    clip_sum[...] = total.astype(BF16)
    total_small = clip_small[0]
    for k in range(1, n_clip):
        total_small = total_small + clip_small[k]
    frame_small[frame] = total_small

    second = []
    for k in range(1, n_frame):
        peer = (frame_peer(k), clip)
        second.append(
            send(
                clip_sum.at[frame_peer(k)],
                frame_recv.at[k - 1],
                f_send.at[0, k],
                f_recv.at[0, k],
                peer,
            )
        )
        second.append(
            send(
                frame_small.at[frame],
                frame_small.at[frame],
                f_send.at[1, k],
                f_recv.at[1, k],
                peer,
            )
        )
    for copy in second:
        copy.wait()
    total = clip_sum[frame].astype(F32)
    for k in range(1, n_frame):
        total = total + frame_recv[k - 1].astype(F32)
    piece[...] = total.astype(BF16)
    total_small = frame_small[0]
    for k in range(1, n_frame):
        total_small = total_small + frame_small[k]
    out_small[...] = total_small
    out_big[clip, frame] = piece[...]

    third = [
        send(
            piece,
            out_big.at[clip, frame],
            a_send.at[k],
            a_recv.at[k],
            (frame_peer(k), clip),
        )
        for k in range(1, n_frame)
    ]
    for copy in third:
        copy.wait()
    fourth = [
        send(
            out_big.at[clip],
            out_big.at[clip],
            z_send.at[k],
            z_recv.at[k],
            (frame, clip_peer(k)),
        )
        for k in range(1, n_clip)
    ]
    for copy in fourth:
        copy.wait()
    for copy in halos:
        copy.wait()


def finish(branch, grads, big, small, n_frame, n_clip):
    rows, width = big.shape
    part = rows // (n_frame * n_clip)
    big = big.reshape(n_clip, n_frame, part, width)
    anywhere = pl.BlockSpec(memory_space=pl.ANY)
    near = pl.BlockSpec(memory_space=pltpu.VMEM)
    dma = pltpu.SemaphoreType.DMA
    return pl.pallas_call(
        functools.partial(finish_kernel, n_frame, n_clip),
        out_shape=[
            jax.ShapeDtypeStruct(branch.shape, BF16),
            jax.ShapeDtypeStruct(grads.shape, BF16),
            jax.ShapeDtypeStruct(big.shape, BF16),
            jax.ShapeDtypeStruct(small.shape, F32),
        ],
        in_specs=[anywhere, anywhere, near, near],
        out_specs=[anywhere, anywhere, near, near],
        scratch_shapes=[
            pltpu.VMEM((n_clip - 1, n_frame, part, width), BF16),
            pltpu.VMEM((n_clip,) + small.shape, F32),
            pltpu.VMEM((n_frame, part, width), BF16),
            pltpu.VMEM((n_frame - 1, part, width), BF16),
            pltpu.VMEM((n_frame,) + small.shape, F32),
            pltpu.VMEM((part, width), BF16),
            dma((2,)),
            dma((2,)),
            dma((2, n_clip)),
            dma((2, n_clip)),
            dma((2, n_frame)),
            dma((2, n_frame)),
            dma((n_frame,)),
            dma((n_frame,)),
            dma((n_clip,)),
            dma((n_clip,)),
        ],
        compiler_params=pltpu.CompilerParams(collective_id=1, has_side_effects=True),
        name="finish",
    )(branch, grads, big, small)


def per_device(
    tokens, lengths, norm_gain, norm_bias, qkv_weight, qkv_bias, proj_weight, proj_bias, grad_out
):
    frames_dev, width = tokens.shape[1], tokens.shape[-1]
    n_frame, n_clip = lax.axis_size("frame"), lax.axis_size("clip")
    first = lax.axis_index("frame") * frames_dev + WT // 2
    scal = jnp.stack(
        [lengths[0], first.astype(jnp.int32), jnp.int32(frames_dev * n_frame), jnp.int32(0)]
    )
    params = (norm_gain, norm_bias, qkv_weight, qkv_bias, proj_weight, proj_bias)
    ahead, ahead_grad = halo(tokens, grad_out, n_frame)
    b_keep, b_send, d_keep, d_send, big, small = compute(
        scal, tokens, ahead, grad_out, ahead_grad, params
    )
    b_got, d_got, big, small = finish(b_send, d_send, big, small, n_frame, n_clip)
    branch_own = jnp.concatenate([b_got, b_keep], axis=1)
    mixed = (tokens.astype(F32) + branch_own.astype(F32)).astype(BF16)
    grad_tokens = grad_out + jnp.concatenate([d_got, d_keep], axis=1)
    big = big.reshape(4, width, width).astype(F32)
    grad_qkv = big[0:3].transpose(1, 0, 2).reshape(width, 3 * width)
    return (
        mixed,
        grad_tokens,
        small[0],
        small[1],
        grad_qkv,
        small[2:5].reshape(3 * width),
        big[3],
        small[5],
    )


def solution(mesh):
    split = P("clip", "frame", None, None, None)
    in_specs = (split, P("clip"), P(), P(), P(), P(), P(), P(), split)
    out_specs = (split, split, P(), P(), P(), P(), P(), P())
    return jax.shard_map(
        per_device, mesh=mesh, in_specs=in_specs, out_specs=out_specs, check_vma=False
    )
```

```python
import functools

import jax
import jax.numpy as jnp
from jax import lax
from jax.experimental import pallas as pl
from jax.experimental.pallas import tpu as pltpu
from jax.sharding import PartitionSpec as P

HEADS = 8
WT = 8
MESH = pl.DeviceIdType.MESH
F32 = jnp.float32
BF16 = jnp.bfloat16


def dot(a, b):
    return jnp.dot(a, b, preferred_element_type=F32)


def dot_nt(a, b):
    return lax.dot_general(a, b, (((1,), (1,)), ((), ())), preferred_element_type=F32)


def compute_kernel(
    patch,
    n_frame,
    scal,
    x_own,
    g_own,
    tokens,
    grads,
    gain,
    nbias,
    wqkv,
    bqkv,
    wproj,
    bproj,
    b_keep,
    d_keep,
    d_send,
    big,
    small,
    b_got,
    ahead,
    b_send,
    in_send,
    in_recv,
    out_send,
    out_recv,
    xs,
    gs,
    wq16,
    wp16,
    mask,
    probs,
    q16,
    k16,
    v16,
    qt16,
    kt16,
    vt16,
    do16,
    dot16,
    acc_o,
    acc_q,
    dkt,
    dvt,
    acc_big,
):
    step = pl.program_id(0)
    half = WT // 2
    padded = xs.shape[1]
    rows = WT * padded
    width = xs.shape[2]
    depth = width // HEADS
    scale = depth ** (-0.5)
    length = scal[0].astype(F32)
    first = scal[1].astype(F32)
    total = scal[2].astype(F32)
    far = F32(-1e9)
    windows = tokens.shape[2]
    frame, clip = lax.axis_index("frame"), lax.axis_index("clip")
    before = (lax.rem(frame + n_frame - 1, n_frame), clip)
    after = (lax.rem(frame + 1, n_frame), clip)

    def incoming(which, w):
        return pltpu.make_async_remote_copy(
            src_ref=(tokens, grads)[which].at[0, 0:half, w],
            dst_ref=ahead.at[which, w],
            send_sem=in_send.at[which, w],
            recv_sem=in_recv.at[which, w],
            device_id=before,
            device_id_type=MESH,
        )

    def outgoing(w):
        return pltpu.make_async_remote_copy(
            src_ref=b_send.at[w],
            dst_ref=b_got.at[0, :, w],
            send_sem=out_send.at[w],
            recv_sem=out_recv.at[w],
            device_id=after,
            device_id_type=MESH,
        )

    @pl.when(step == 0)
    def _():
        barrier = pltpu.get_barrier_semaphore()
        for peer in (before, after):
            pl.semaphore_signal(barrier, inc=1, device_id=peer, device_id_type=MESH)
        pl.semaphore_wait(barrier, 2)
        for w in range(windows):
            for which in range(2):
                incoming(which, w).start()

    def frame_of(index):
        row = index.astype(F32)
        slot = jnp.floor((row + 0.5) * (1.0 / padded))
        time = first + slot
        time = jnp.where(time >= total, time - total, time)
        return time, row - slot * padded

    t_col, in_col = frame_of(lax.broadcasted_iota(jnp.int32, (rows, 1), 0))
    valid_col = jnp.where(t_col < length, 1.0, 0.0).astype(F32)

    @pl.when(step == 0)
    def _():
        xs[...] = jnp.zeros_like(xs)
        gs[...] = jnp.zeros_like(gs)
        wq16[...] = wqkv[...].astype(BF16)
        wp16[...] = wproj[...].astype(BF16)
        acc_big[...] = jnp.zeros_like(acc_big)
        small[...] = jnp.zeros_like(small)
        t_row, in_row = frame_of(lax.broadcasted_iota(jnp.int32, (1, rows), 1))
        key_bias = jnp.where((t_row < length) & (in_row < patch), 0.0, far)
        region_row = jnp.where(t_row < half, 1.0, 0.0)
        region_col = jnp.where(t_col < half, 1.0, 0.0)
        mask[...] = key_bias + jnp.where(region_col == region_row, 0.0, far)

    xs[0:half, 0:patch, :] = x_own[0, :, 0].astype(F32)
    gs[0:half, 0:patch, :] = g_own[0, :, 0].astype(F32)
    incoming(0, step).wait()
    xs[half:WT, 0:patch, :] = ahead[0, step].astype(F32)

    x = xs[...].reshape(rows, width)
    mean = jnp.sum(x, axis=-1, keepdims=True) * (1.0 / width)
    xc = x - mean
    var = jnp.sum(xc * xc, axis=-1, keepdims=True) * (1.0 / width)
    inv = lax.rsqrt(var + 1e-05)
    normed_f = (xc * inv * gain[...] + nbias[...]).astype(BF16).astype(F32)
    normed = normed_f.astype(BF16)
    normed_t = normed_f.T.astype(BF16)
    for part, (ref, ref_t) in enumerate(((q16, qt16), (k16, kt16), (v16, vt16))):
        cols = slice(part * width, (part + 1) * width)
        value = dot(normed, wq16[:, cols]) + bqkv[:, cols]
        rounded = value.astype(BF16)
        ref[...] = rounded
        ref_t[...] = rounded.astype(F32).T.astype(BF16)

    lane_head = lax.broadcasted_iota(jnp.int32, (1, width), 1) // depth
    row_head = lax.broadcasted_iota(jnp.int32, (width, 1), 0) // depth
    zero16 = jnp.zeros((), BF16)

    acc_o[...] = jnp.zeros_like(acc_o)

    def forward(h, carry):
        row_on = jnp.where(row_head == h, 1.0, 0.0).astype(BF16)
        lane_on = jnp.where(lane_head == h, 1.0, 0.0).astype(BF16)
        scores = dot(q16[...], kt16[...] * row_on) * scale + mask[...]
        top = jnp.max(scores, axis=-1, keepdims=True)
        e = jnp.exp(scores - top)
        p = (e * (1.0 / jnp.sum(e, axis=-1, keepdims=True))).astype(BF16)
        probs[h] = p
        acc_o[...] += dot(p, v16[...] * lane_on)
        return carry

    lax.fori_loop(0, HEADS, forward, 0, unroll=2)
    att = acc_o[...].astype(BF16)
    att_f = att.astype(F32)
    projected = (dot(att, wp16[...]) + bproj[...]) * valid_col
    projected = projected.reshape(WT, padded, width)
    b_keep[0, :, 0] = projected[0:half, 0:patch].astype(BF16)
    b_send[step] = projected[half:WT, 0:patch].astype(BF16)
    outgoing(step).start()
    incoming(1, step).wait()
    gs[half:WT, 0:patch, :] = ahead[1, step].astype(F32)

    g = gs[...].reshape(rows, width) * valid_col
    g_16 = g.astype(BF16)
    small[5:6, :] += jnp.sum(g, axis=0, keepdims=True)
    acc_big[:, 3 * width : 4 * width] += dot(att_f.T.astype(BF16), g_16)
    d_att = dot_nt(g_16, wp16[...]).astype(BF16)
    do16[...] = d_att
    d_att_f = d_att.astype(F32)
    dot16[...] = d_att_f.T.astype(BF16)
    acc_o[...] = d_att_f * att_f
    acc_q[...] = jnp.zeros_like(acc_q)

    def backward(h, carry):
        row_on = jnp.where(row_head == h, 1.0, 0.0).astype(BF16)
        lane_on = jnp.where(lane_head == h, 1.0, 0.0).astype(BF16)
        delta = jnp.sum(
            jnp.where(lane_head == h, acc_o[...], 0.0), axis=-1, keepdims=True
        )
        p = probs[h]
        dp = dot(do16[...], vt16[...] * row_on)
        ds = (p.astype(F32) * (dp - delta)).astype(BF16)
        acc_q[...] += dot(ds, k16[...] * lane_on)
        at = pl.ds(pl.multiple_of(h * depth, depth), depth)
        dkt[at, :] = dot(qt16[at, :], ds)
        dvt[at, :] = dot(dot16[at, :], p)
        return carry

    lax.fori_loop(0, HEADS, backward, 0, unroll=2)
    d_normed = jnp.zeros((rows, width), F32)
    for part in range(3):
        if part == 0:
            d_part = acc_q[...] * scale
        elif part == 1:
            d_part = dkt[...].T * scale
        else:
            d_part = dvt[...].T
        d_16 = d_part.astype(BF16)
        cols = slice(part * width, (part + 1) * width)
        small[2 + part : 3 + part, :] += jnp.sum(d_16.astype(F32), axis=0, keepdims=True)
        acc_big[:, cols] += dot(normed_t, d_16)
        d_normed = d_normed + dot_nt(d_16, wq16[:, cols])
    dn = d_normed.astype(BF16).astype(F32)
    x = xs[...].reshape(rows, width)
    xhat = (x - mean) * inv
    small[0:1, :] += jnp.sum(dn * xhat, axis=0, keepdims=True)
    small[1:2, :] += jnp.sum(dn, axis=0, keepdims=True)
    dh = dn * gain[...]
    m1 = jnp.sum(dh, axis=-1, keepdims=True) * (1.0 / width)
    m2 = jnp.sum(dh * xhat, axis=-1, keepdims=True) * (1.0 / width)
    dx = (inv * (dh - m1 - xhat * m2)).reshape(WT, padded, width)
    d_keep[0, :, 0] = dx[0:half, 0:patch].astype(BF16)
    d_send[0, :, 0] = dx[half:WT, 0:patch].astype(BF16)

    @pl.when(step == pl.num_programs(0) - 1)
    def _():
        big[...] = acc_big[...].astype(BF16)
        for w in range(windows):
            outgoing(w).wait()


def compute(scal, tokens, grad_out, params, n_frame):
    gain, nbias, wqkv, bqkv, wproj, bproj = params
    _, frames, windows, patch, width = tokens.shape
    half = WT // 2
    padded = -(-patch // 8) * 8
    rows = WT * padded
    own = pl.BlockSpec((1, half, 1, patch, width), lambda w: (0, 1, w, 0, 0))
    other = pl.BlockSpec((1, half, 1, patch, width), lambda w: (0, 0, w, 0, 0))

    def whole(shape):
        return pl.BlockSpec(shape, lambda w: (0,) * len(shape))

    half_shape = jax.ShapeDtypeStruct((1, half, windows, patch, width), BF16)
    tall = pltpu.VMEM((rows, width), BF16)
    wide = pltpu.VMEM((width, rows), BF16)
    return pl.pallas_call(
        functools.partial(compute_kernel, patch, n_frame),
        grid=(windows,),
        out_shape=[half_shape] * 3
        + [
            jax.ShapeDtypeStruct((width, 4 * width), BF16),
            jax.ShapeDtypeStruct((8, width), F32),
            half_shape,
        ],
        in_specs=[
            pl.BlockSpec(memory_space=pltpu.SMEM),
            own,
            own,
            pl.BlockSpec(memory_space=pl.ANY),
            pl.BlockSpec(memory_space=pl.ANY),
            whole((1, width)),
            whole((1, width)),
            whole((width, 3 * width)),
            whole((1, 3 * width)),
            whole((width, width)),
            whole((1, width)),
        ],
        out_specs=[other] * 3
        + [
            whole((width, 4 * width)),
            whole((8, width)),
            pl.BlockSpec(memory_space=pl.ANY),
        ],
        scratch_shapes=[
            pltpu.VMEM((2, windows, half, patch, width), BF16),
            pltpu.VMEM((windows, half, patch, width), BF16),
            pltpu.SemaphoreType.DMA((2, windows)),
            pltpu.SemaphoreType.DMA((2, windows)),
            pltpu.SemaphoreType.DMA((windows,)),
            pltpu.SemaphoreType.DMA((windows,)),
            pltpu.VMEM((WT, padded, width), F32),
            pltpu.VMEM((WT, padded, width), F32),
            pltpu.VMEM((width, 3 * width), BF16),
            pltpu.VMEM((width, width), BF16),
            pltpu.VMEM((rows, rows), F32),
            pltpu.VMEM((HEADS, rows, rows), BF16),
            tall,
            tall,
            tall,
            wide,
            wide,
            wide,
            tall,
            wide,
            pltpu.VMEM((rows, width), F32),
            pltpu.VMEM((rows, width), F32),
            pltpu.VMEM((width, rows), F32),
            pltpu.VMEM((width, rows), F32),
            pltpu.VMEM((width, 4 * width), F32),
        ],
        compiler_params=pltpu.CompilerParams(
            dimension_semantics=("arbitrary",),
            vmem_limit_bytes=56 * 2**20,
            collective_id=0,
            has_side_effects=True,
        ),
        name="window_attention",
    )(
        scal,
        tokens,
        grad_out,
        tokens,
        grad_out,
        gain.reshape(1, width),
        nbias.reshape(1, width),
        wqkv,
        bqkv.reshape(1, 3 * width),
        wproj,
        bproj.reshape(1, width),
    )


def finish_kernel(
    n_frame,
    n_clip,
    grads,
    big,
    small,
    got_grads,
    out_big,
    out_small,
    clip_recv,
    clip_small,
    clip_sum,
    frame_recv,
    frame_small,
    piece,
    h_send,
    h_recv,
    c_send,
    c_recv,
    f_send,
    f_recv,
    a_send,
    a_recv,
    z_send,
    z_recv,
):
    frame, clip = lax.axis_index("frame"), lax.axis_index("clip")
    after = lax.rem(frame + 1, n_frame)
    barrier = pltpu.get_barrier_semaphore()

    def frame_peer(k):
        return lax.rem(frame + k, n_frame)

    def clip_peer(k):
        return lax.rem(clip + k, n_clip)

    for k in range(1, n_clip):
        pl.semaphore_signal(
            barrier, inc=1, device_id=(frame, clip_peer(k)), device_id_type=MESH
        )
    for k in range(1, n_frame):
        pl.semaphore_signal(
            barrier, inc=1, device_id=(frame_peer(k), clip), device_id_type=MESH
        )
    pl.semaphore_wait(barrier, n_clip + n_frame - 2)

    def send(src, dst, s, r, peer):
        copy = pltpu.make_async_remote_copy(
            src_ref=src,
            dst_ref=dst,
            send_sem=s,
            recv_sem=r,
            device_id=peer,
            device_id_type=MESH,
        )
        copy.start()
        return copy

    first = []
    for k in range(1, n_clip):
        peer = (frame, clip_peer(k))
        first.append(
            send(big.at[clip_peer(k)], clip_recv.at[k - 1], c_send.at[0, k], c_recv.at[0, k], peer)
        )
        first.append(send(small, clip_small.at[clip], c_send.at[1, k], c_recv.at[1, k], peer))
    halos = [send(grads, got_grads, h_send.at[0], h_recv.at[0], (after, clip))]
    clip_small[clip] = small[...]
    for copy in first:
        copy.wait()
    total = big[clip].astype(F32)
    for k in range(1, n_clip):
        total = total + clip_recv[k - 1].astype(F32)
    clip_sum[...] = total.astype(BF16)
    total_small = clip_small[0]
    for k in range(1, n_clip):
        total_small = total_small + clip_small[k]
    frame_small[frame] = total_small

    second = []
    for k in range(1, n_frame):
        peer = (frame_peer(k), clip)
        second.append(
            send(
                clip_sum.at[frame_peer(k)],
                frame_recv.at[k - 1],
                f_send.at[0, k],
                f_recv.at[0, k],
                peer,
            )
        )
        second.append(
            send(
                frame_small.at[frame],
                frame_small.at[frame],
                f_send.at[1, k],
                f_recv.at[1, k],
                peer,
            )
        )
    for copy in second:
        copy.wait()
    total = clip_sum[frame].astype(F32)
    for k in range(1, n_frame):
        total = total + frame_recv[k - 1].astype(F32)
    piece[...] = total.astype(BF16)
    total_small = frame_small[0]
    for k in range(1, n_frame):
        total_small = total_small + frame_small[k]
    out_small[...] = total_small
    out_big[clip, frame] = piece[...]

    third = [
        send(
            piece,
            out_big.at[clip, frame],
            a_send.at[k],
            a_recv.at[k],
            (frame_peer(k), clip),
        )
        for k in range(1, n_frame)
    ]
    for copy in third:
        copy.wait()
    fourth = [
        send(
            out_big.at[clip],
            out_big.at[clip],
            z_send.at[k],
            z_recv.at[k],
            (frame, clip_peer(k)),
        )
        for k in range(1, n_clip)
    ]
    for copy in fourth:
        copy.wait()
    for copy in halos:
        copy.wait()


def finish(grads, big, small, n_frame, n_clip):
    rows, width = big.shape
    part = rows // (n_frame * n_clip)
    big = big.reshape(n_clip, n_frame, part, width)
    anywhere = pl.BlockSpec(memory_space=pl.ANY)
    near = pl.BlockSpec(memory_space=pltpu.VMEM)
    dma = pltpu.SemaphoreType.DMA
    return pl.pallas_call(
        functools.partial(finish_kernel, n_frame, n_clip),
        out_shape=[
            jax.ShapeDtypeStruct(grads.shape, BF16),
            jax.ShapeDtypeStruct(big.shape, BF16),
            jax.ShapeDtypeStruct(small.shape, F32),
        ],
        in_specs=[anywhere, near, near],
        out_specs=[anywhere, near, near],
        scratch_shapes=[
            pltpu.VMEM((n_clip - 1, n_frame, part, width), BF16),
            pltpu.VMEM((n_clip,) + small.shape, F32),
            pltpu.VMEM((n_frame, part, width), BF16),
            pltpu.VMEM((n_frame - 1, part, width), BF16),
            pltpu.VMEM((n_frame,) + small.shape, F32),
            pltpu.VMEM((part, width), BF16),
            dma((1,)),
            dma((1,)),
            dma((2, n_clip)),
            dma((2, n_clip)),
            dma((2, n_frame)),
            dma((2, n_frame)),
            dma((n_frame,)),
            dma((n_frame,)),
            dma((n_clip,)),
            dma((n_clip,)),
        ],
        compiler_params=pltpu.CompilerParams(collective_id=1, has_side_effects=True),
        name="finish",
    )(grads, big, small)


def per_device(
    tokens, lengths, norm_gain, norm_bias, qkv_weight, qkv_bias, proj_weight, proj_bias, grad_out
):
    frames_dev, width = tokens.shape[1], tokens.shape[-1]
    n_frame, n_clip = lax.axis_size("frame"), lax.axis_size("clip")
    first = lax.axis_index("frame") * frames_dev + WT // 2
    scal = jnp.stack(
        [lengths[0], first.astype(jnp.int32), jnp.int32(frames_dev * n_frame), jnp.int32(0)]
    )
    params = (norm_gain, norm_bias, qkv_weight, qkv_bias, proj_weight, proj_bias)
    b_keep, d_keep, d_send, big, small, b_got = compute(scal, tokens, grad_out, params, n_frame)
    d_got, big, small = finish(d_send, big, small, n_frame, n_clip)
    branch_own = jnp.concatenate([b_got, b_keep], axis=1)
    mixed = (tokens.astype(F32) + branch_own.astype(F32)).astype(BF16)
    grad_tokens = grad_out + jnp.concatenate([d_got, d_keep], axis=1)
    big = big.reshape(width, 4 * width).astype(F32)
    return (
        mixed,
        grad_tokens,
        small[0],
        small[1],
        big[:, : 3 * width],
        small[2:5].reshape(3 * width),
        big[:, 3 * width :],
        small[5],
    )


def solution(mesh):
    split = P("clip", "frame", None, None, None)
    in_specs = (split, P("clip"), P(), P(), P(), P(), P(), P(), split)
    out_specs = (split, split, P(), P(), P(), P(), P(), P())
    return jax.shard_map(
        per_device, mesh=mesh, in_specs=in_specs, out_specs=out_specs, check_vma=False
    )
```
